256 devices in a mesh: pb: 8 (over z), freq: 4 (over y_hi, core), ga: 8 (over x, y_lo).
Axes of the slice: x: 4, y: 4 (y_hi: 2, y_lo: 2; y = y_hi * 2 + y_lo), z: 8, core: 2. Of those that a mesh axis runs over, the one named last changes fastest.
Arguments:
- densities: bfloat16 [8, 2, 256, 4096], P('pb', None, ('freq', 'ga')), may hold values from -0.5 to 0.5
- screened: bfloat16 [8, 4, 2, 4096, 4096], P('pb', 'freq', None, 'ga'), may hold values from -0.09375 to 0.09375
- energies: float32 [32, 256], replicated, may hold values from -2.5 to 2.5
- occupied: int32 [32], replicated, may hold values from 64 to 192
- kmq: int32 [8], replicated, may hold values from 0 to 31
- offsets: int32 [4], replicated, may hold values from -32 to 31
- weights: float32 [4], replicated, may hold values from 0.5 to 2
Outputs:
- sigma: float32 [2, 1, 128], P(None, None, ('pb', 'freq'))
The draws below stay inside these ranges and needn't reach their ends.
All inputs are finite; a program needn't handle non-finite values.
Results may differ from the reference program's by a relative error of at most 0.0003.
Values may be sent and summed in bfloat16 or wider, within the bound.
No kernel may reach another device: no remote copies, remote signals or barrier semaphores. Data moves between devices by JAX's collectives and lax.ppermute only.
A program may use at most 64 MiB of HBM per device.

```python
import math
import jax
import jax.numpy as jnp
from jax import lax

G = 4096
NB = 256
NS = 1
Q = 8
NKP = 32
NW = 4
NOUT = 128
K = 256


def place_ends(result, stream_key, least, high):
    longest = result.shape.index(max(result.shape))
    spots = []
    for shift in (0, 1):
        where = [jax.random.randint(jax.random.fold_in(stream_key, axis), (), 0, length) for axis, length in enumerate(result.shape)]
        where[longest] = (where[longest] + shift) % result.shape[longest]
        spots.append(tuple(where))
    return result.at[spots[0]].set(least).at[spots[1]].set(high)


def block_scale(rng, shape, split, least, top_value):
    def one(dim, blocks):
        steps = jax.random.uniform(jax.random.fold_in(jax.random.fold_in(rng, 6), dim), (blocks,), jnp.float32, least / len(split), top_value / len(split))
        return jnp.repeat(jnp.exp(steps), shape[dim] // blocks).reshape((-1,) + (1,) * (len(shape) - dim - 1))

    factor_of = one(*split[0])
    for cut in split[1:]:
        factor_of = factor_of * one(*cut)
    return factor_of


def centred(key, shape, width, reach, pieces=(), kind=jnp.bfloat16):
    result = width * jax.random.normal(key, shape, jnp.float32)
    if pieces:
        result = result * block_scale(key, shape, pieces, -0.22, 0.18)
    return jnp.clip(result, -reach, reach).astype(kind)


def setup_inputs(seed: int = 0) -> dict:
    key_list = jax.random.split(jax.random.key(seed), 8)
    return {
        "densities": centred(key_list[0], (Q, 2, K, G), (0.7071 * G ** -0.25), 0.5, ((0, 8), (2, 32))),
        "screened": centred(key_list[1], (Q, NW, 2, G, G), G ** -0.5, 0.09375, ((0, 8), (1, 4), (3, 8))),
        "energies": jnp.clip(jax.random.uniform(key_list[2], (NKP, NB), jnp.float32, -2.5, 2.5), -2.5, 2.5),
        "occupied": place_ends(jax.random.randint(key_list[3], (NKP,), NB // 4, 3 * NB // 4 + 1), jax.random.fold_in(key_list[3], 1), NB // 4, (3 * NB // 4 + 1) - 1).astype(jnp.int32),
        "kmq": place_ends(jax.random.randint(key_list[4], (Q,), 0, NKP), jax.random.fold_in(key_list[4], 1), 0, NKP - 1).astype(jnp.int32),
        "offsets": place_ends(jax.random.randint(key_list[5], (NW,), 0 - NOUT // 4, NOUT // 4), jax.random.fold_in(key_list[5], 1), 0 - NOUT // 4, (NOUT // 4) - 1).astype(jnp.int32),
        "weights": jnp.clip(jnp.exp(jax.random.uniform(key_list[6], (NW,), jnp.float32, math.log(0.5), math.log(2.0))), 0.5, 2.0),
    }


broadening = 0.15


def green_parts(level_row, filled, freq_shift, omegas):
    bands = jnp.arange(level_row.shape[0], dtype=jnp.int32)
    pole_sign = jnp.where(bands < filled, -1.0, 1.0).astype(jnp.float32)
    real_part = omegas[None, :] - freq_shift - level_row[:, None]
    imag_part = broadening * pole_sign[:, None]
    denominator = real_part * real_part + imag_part * imag_part
    return real_part / denominator, -imag_part / denominator


def spectrum(pair_real, pair_imag, green_real, green_imag):
    exact = lax.Precision.HIGHEST
    real_out = jnp.dot(pair_real, green_real, precision=exact) - jnp.dot(pair_imag, green_imag, precision=exact)
    imag_out = jnp.dot(pair_real, green_imag, precision=exact) + jnp.dot(pair_imag, green_real, precision=exact)
    return real_out, imag_out


def pair_sums(density, screen):
    pair_rows = density.shape[1]
    basis_rows = screen.shape[1]
    product = lax.dot_general(density.reshape(2 * pair_rows, -1), screen.reshape(2 * basis_rows, -1),
                              (((1,), (1,)), ((), ())), preferred_element_type=jnp.float32)
    product = product.reshape(2, pair_rows, 2, basis_rows)
    real_x = product[0, :, 0] - product[1, :, 1]
    imag_x = product[0, :, 1] + product[1, :, 0]
    dense = density.astype(jnp.float32)
    real_sum = jnp.sum(dense[0] * real_x + dense[1] * imag_x, axis=1)
    imag_sum = jnp.sum(dense[0] * imag_x - dense[1] * real_x, axis=1)
    return real_sum, imag_sum


def reference(densities, screened, energies, occupied, kmq, offsets, weights):
    omegas = -2.0 + 4.0 * jnp.arange(NOUT, dtype=jnp.float32) / NOUT
    summed_real = jnp.zeros((NS, NOUT), jnp.float32)
    summed_imag = jnp.zeros((NS, NOUT), jnp.float32)
    for qpoint in range(Q):
        kpoint = kmq[qpoint]
        level_row = energies[kpoint]
        filled = occupied[kpoint]
        for frequency in range(NW):
            real_sum, imag_sum = pair_sums(densities[qpoint], screened[qpoint, frequency])
            weight_now = weights[frequency]
            real_sum = (weight_now * real_sum).reshape(NS, NB)
            imag_sum = (weight_now * imag_sum).reshape(NS, NB)
            freq_shift = 4.0 * offsets[frequency].astype(jnp.float32) / NOUT
            green_real, green_imag = green_parts(level_row, filled, freq_shift, omegas)
            real_out, imag_out = spectrum(real_sum, imag_sum, green_real, green_imag)
            summed_real = summed_real + real_out
            summed_imag = summed_imag + imag_out
    prefactor = 1.0 / (2.0 * math.pi * Q)
    return jnp.stack([-prefactor * summed_imag, prefactor * summed_real])
```

```python
import math

import jax
import jax.numpy as jnp
from jax import lax
from jax.sharding import Mesh
from jax.sharding import PartitionSpec as P

AXES = ("pb", "yh", "core", "x", "yl")
OFFSETS = (2, 1, -1)
BROADENING = 0.15


def position(z, y, core, x):
    return (((z * 2 + y // 2) * 2 + core) * 4 + x) * 2 + y % 2


def moved(value, count_pb, place):
    pairs = []
    for z in range(count_pb):
        for y in range(4):
            for core in range(2):
                for x in range(4):
                    ny, ncore, nx = place(y, core, x)
                    pairs.append(
                        (position(z, y, core, x), position(z, ny % 4, ncore, nx % 4))
                    )
    return lax.ppermute(value, AXES, pairs)


def along_first(step):
    return lambda y, core, x: (y, core, x + step) if core == 0 else (y + step, core, x)


def along_second(step):
    return lambda y, core, x: (y + step, core, x) if core == 0 else (y, core, x + step)


def other_core(y, core, x):
    return (y, 1 - core, x)


def pair_sums(blocks, screen, panel):
    count, _, rows, width = blocks.shape
    panel_rows = screen.shape[1]
    product = lax.dot_general(
        blocks.reshape(count * 2 * rows, width),
        screen.reshape(2 * panel_rows, width),
        (((1,), (1,)), ((), ())),
        preferred_element_type=jnp.float32,
    ).reshape(count, 2, rows, 2, panel_rows)
    real_x = product[:, 0, :, 0] - product[:, 1, :, 1]
    imag_x = product[:, 0, :, 1] + product[:, 1, :, 0]
    own = lax.dynamic_slice_in_dim(blocks, panel * panel_rows, panel_rows, 3)
    own = own.astype(jnp.float32)
    real_sum = jnp.sum(own[:, 0] * real_x + own[:, 1] * imag_x, axis=-1)
    imag_sum = jnp.sum(own[:, 0] * imag_x - own[:, 1] * real_x, axis=-1)
    return real_sum, imag_sum


def green_parts(levels, filled, freq_shift, omegas):
    pole_sign = jnp.where(filled, -1.0, 1.0).astype(jnp.float32)
    real_part = omegas - freq_shift - levels[..., None]
    imag_part = BROADENING * pole_sign[..., None]
    denominator = real_part * real_part + imag_part * imag_part
    return real_part / denominator, -imag_part / denominator


def body(densities, screened, energies, occupied, kmq, offsets, weights):
    count_pb = lax.axis_size("pb")
    z = lax.axis_index("pb")
    yh = lax.axis_index("yh")
    core = lax.axis_index("core")
    x = lax.axis_index("x")
    yl = lax.axis_index("yl")
    y = yh * 2 + yl
    panel = x * 2 + yl
    block = densities[0]
    screen = screened[0, 0]
    rows = block.shape[1]

    swapped = moved(screen, count_pb, other_core)
    first = [moved(block, count_pb, along_first(s)) for s in OFFSETS]
    second = [moved(block, count_pb, along_second(s)) for s in OFFSETS]
    line = jnp.stack(first)
    rest = [moved(line, count_pb, along_second(s)) for s in OFFSETS]

    near = jnp.stack([block, *first, *second])
    far = jnp.concatenate(rest)
    from_first = [0] + [-s for s in OFFSETS] + [0] * 3 + [-s for s in OFFSETS] * 3
    from_second = [0] * 4 + [-s for s in OFFSETS] + [-s for s in OFFSETS for _ in OFFSETS]
    a = jnp.array(from_first)
    b = jnp.array(from_second)
    source_x = (x + jnp.where(core == 0, a, b)) % 4
    source_y = (y + jnp.where(core == 0, b, a)) % 4
    source = (source_y // 2 * 2 + core) * 8 + source_x * 2 + source_y % 2

    kpoint = kmq[z]
    bands = source[:, None] * rows + jnp.arange(rows)
    levels = energies[kpoint].reshape(-1, rows)[source]
    filled = bands < occupied[kpoint]
    total_out = 4 * count_pb * 4
    omegas = -2.0 + 4.0 * jnp.arange(total_out, dtype=jnp.float32) / total_out

    spectrum = jnp.zeros((2, total_out), jnp.float32)
    for freq, panel_of in ((yh * 2 + core, screen), (yh * 2 + 1 - core, swapped)):
        near_sums = pair_sums(near, panel_of, panel)
        far_sums = pair_sums(far, panel_of, panel)
        real_sum = jnp.concatenate([near_sums[0], far_sums[0]])[..., None]
        imag_sum = jnp.concatenate([near_sums[1], far_sums[1]])[..., None]
        freq_shift = 4.0 * offsets[freq].astype(jnp.float32) / total_out
        green_real, green_imag = green_parts(levels, filled, freq_shift, omegas)
        real_out = jnp.sum(real_sum * green_real - imag_sum * green_imag, axis=(0, 1))
        imag_out = jnp.sum(real_sum * green_imag + imag_sum * green_real, axis=(0, 1))
        spectrum = spectrum + weights[freq] * jnp.stack([real_out, imag_out])

    devices = count_pb * 32
    sent = jnp.broadcast_to(spectrum, (devices, 2, total_out))
    parts = lax.all_to_all(sent, AXES, 0, 0, tiled=True)
    total = jnp.sum(parts, axis=0)
    slot = (z * 2 + yh) * 2 + core
    mine = lax.dynamic_slice_in_dim(total, slot * 4, 4, 1)
    prefactor = 1.0 / (2.0 * math.pi * count_pb)
    return jnp.stack([-prefactor * mine[1:2], prefactor * mine[0:1]])


def solution(mesh):
    torus = Mesh(mesh.devices.reshape(mesh.shape["pb"], 2, 2, 4, 2), AXES)
    return jax.shard_map(
        body,
        mesh=torus,
        in_specs=(
            P("pb", None, ("yh", "core", "x", "yl"), None),
            P("pb", ("yh", "core"), None, ("x", "yl"), None),
            P(),
            P(),
            P(),
            P(),
            P(),
        ),
        out_specs=P(None, None, ("pb", "yh", "core")),
        check_vma=False,
    )
```

```python
import functools
import math

import jax
import jax.numpy as jnp
from jax import lax
from jax.experimental import pallas as pl
from jax.experimental.pallas import tpu as pltpu
from jax.sharding import Mesh
from jax.sharding import PartitionSpec as P

AXES = ("pb", "yh", "core", "x", "yl")
SAME_CORE = ("pb", "yh", "x", "yl")
OFFSETS = (2, 1, -1)
FIRST_OF = (0, -2, -1, 1) + (0, 0, 0) + (-2, -1, 1) * 3
SECOND_OF = (0, 0, 0, 0) + (-2, -1, 1) + (-2,) * 3 + (-1,) * 3 + (1,) * 3
NEAR = 7
BROADENING = 0.15
TILE = 512


def position(z, y, core, x):
    return (((z * 2 + y // 2) * 2 + core) * 4 + x) * 2 + y % 2


def moved(value, count_pb, place):
    pairs = []
    for z in range(count_pb):
        for y in range(4):
            for core in range(2):
                for x in range(4):
                    ny, ncore, nx = place(y, core, x)
                    pairs.append(
                        (position(z, y, core, x), position(z, ny % 4, ncore, nx % 4))
                    )
    return lax.ppermute(value, AXES, pairs)


def along_first(step):
    return lambda y, core, x: (y, core, x + step) if core == 0 else (y + step, core, x)


def along_second(step):
    return lambda y, core, x: (y + step, core, x) if core == 0 else (y, core, x + step)


def other_core(y, core, x):
    return (y, 1 - core, x)


def place_of_device():
    return [lax.axis_index(name) for name in AXES]


def stacked_rows(blocks, part, start, width):
    pieces = [ref[k, part, :, pl.ds(start, width)].astype(jnp.float32) for ref, k in blocks]
    return jnp.concatenate(pieces, axis=0)


def fill_left(blocks, left_ref, panel, panel_rows):
    start = pl.multiple_of(panel * panel_rows, panel_rows)
    real = stacked_rows(blocks, 0, start, panel_rows)
    imag = stacked_rows(blocks, 1, start, panel_rows)
    half = real.shape[0]
    left_ref[:half, :panel_rows] = real.astype(jnp.bfloat16)
    left_ref[:half, panel_rows:] = imag.astype(jnp.bfloat16)
    left_ref[half:, :panel_rows] = (-imag).astype(jnp.bfloat16)
    left_ref[half:, panel_rows:] = real.astype(jnp.bfloat16)


def add_tile(blocks, left_ref, screen_ref, tile, sums):
    start = pl.multiple_of(tile * TILE, TILE)
    half = left_ref.shape[0] // 2
    right = screen_ref[:, :, pl.ds(start, TILE)].reshape(left_ref.shape[1], TILE)
    product = jnp.dot(left_ref[...], right, preferred_element_type=jnp.float32)
    y_real, y_imag = product[:half], product[half:]
    real = stacked_rows(blocks, 0, start, TILE)
    imag = stacked_rows(blocks, 1, start, TILE)
    terms = (real * y_real - imag * y_imag, real * y_imag + imag * y_real)
    out = []
    for held, term in zip(sums, terms):
        for k in range(TILE // 128):
            held = held + term[:, k * 128 : (k + 1) * 128]
        out.append(held)
    return tuple(out)


def near_kernel(
    kmq_hbm,
    occupied_hbm,
    offsets_hbm,
    weights_hbm,
    energies_hbm,
    block_hbm,
    own_hbm,
    a0_ref,
    a1_ref,
    a2_ref,
    b0_ref,
    b1_ref,
    b2_ref,
    swap_ref,
    own_ref,
    green_ref,
    spectrum_ref,
    kmq_ref,
    occupied_ref,
    offsets_ref,
    weights_ref,
    energies_ref,
    block_ref,
    left_ref,
    sems,
):
    z, yh, core, x, yl = place_of_device()
    y = yh * 2 + yl
    panel_rows, width = own_hbm.shape[1:]
    tiles = width // TILE
    small = [
        pltpu.make_async_copy(src, dst, sems.at[tiles + k])
        for k, (src, dst) in enumerate(
            (
                (kmq_hbm, kmq_ref),
                (occupied_hbm, occupied_ref),
                (offsets_hbm, offsets_ref),
                (weights_hbm, weights_ref),
                (energies_hbm, energies_ref),
                (block_hbm, block_ref),
            )
        )
    ]
    large = []
    for tile in range(tiles):
        piece = pl.ds(tile * TILE, TILE)
        large.append(
            pltpu.make_async_copy(
                own_hbm.at[:, :, piece], own_ref.at[:, :, piece], sems.at[tile]
            )
        )
    for copy in small + large:
        copy.start()
    for copy in small:
        copy.wait()

    kpoint = kmq_ref[z]
    level_row = energies_ref[pl.ds(kpoint, 1), :]
    filled = occupied_ref[kpoint]
    rows = block_ref.shape[2]
    lanes = level_row.shape[1]
    columns, signs = [], []
    for first, second in zip(FIRST_OF, SECOND_OF):
        source_x = (x + jnp.where(core == 0, first, second) + 4) % 4
        source_y = (y + jnp.where(core == 0, second, first) + 4) % 4
        source = (source_y // 2 * 2 + core) * 8 + source_x * 2 + source_y % 2
        band = source * rows + lax.broadcasted_iota(jnp.int32, (rows, lanes), 0)
        match = lax.broadcasted_iota(jnp.int32, (rows, lanes), 1) == band
        picked = jnp.where(match, jnp.broadcast_to(level_row, (rows, lanes)), 0.0)
        columns.append(jnp.sum(picked, axis=1, keepdims=True))
        signs.append(jnp.where(band[:, :1] < filled, -1.0, 1.0))
    levels = jnp.concatenate(columns, axis=0)
    imag_part = BROADENING * jnp.concatenate(signs, axis=0)

    total_out = 128
    count = levels.shape[0]
    lane = lax.broadcasted_iota(jnp.int32, (count, total_out), 1)
    is_real = lane < 64
    within = lane % 64
    for k in range(2):
        freq = yh * 2 + jnp.where(k == 0, core, 1 - core)
        freq_shift = 4.0 * offsets_ref[freq].astype(jnp.float32) / total_out
        weight = weights_ref[freq]
        for target in range(2):
            index = (within // 4 * 2 + target) * 4 + within % 4
            omegas = -2.0 + 4.0 * index.astype(jnp.float32) / total_out
            real_part = omegas - freq_shift - levels
            denominator = real_part * real_part + imag_part * imag_part
            g_real = weight * (real_part / denominator)
            g_imag = weight * (-imag_part / denominator)
            green_ref[k, target, 0] = jnp.where(is_real, g_real, g_imag)
            green_ref[k, target, 1] = jnp.where(is_real, -g_imag, g_real)

    blocks = [
        (ref, 0)
        for ref in (block_ref, a0_ref, a1_ref, a2_ref, b0_ref, b1_ref, b2_ref)
    ]
    fill_left(blocks, left_ref, x * 2 + yl, panel_rows)
    half = left_ref.shape[0] // 2
    total = [jnp.zeros((1, total_out), jnp.float32) for _ in range(2)]
    for k, screen_ref in ((1, swap_ref), (0, own_ref)):
        sums = (jnp.zeros((half, 128), jnp.float32),) * 2
        for tile in range(tiles):
            if k == 0:
                large[tile].wait()
            sums = add_tile(blocks, left_ref, screen_ref, tile, sums)
        total = added(total, sums, green_ref, k, 0, half)
    spectrum_ref[0:1, :] = total[0]
    spectrum_ref[1:2, :] = total[1]


def added(total, sums, green_ref, k, begin, half):
    p_real = jnp.sum(sums[0], axis=1, keepdims=True)
    p_imag = jnp.sum(sums[1], axis=1, keepdims=True)
    out = []
    for target in range(2):
        u = green_ref[k, target, 0, begin : begin + half]
        v = green_ref[k, target, 1, begin : begin + half]
        out.append(total[target] + jnp.sum(p_real * u + p_imag * v, axis=0, keepdims=True))
    return out


def far_kernel(
    spectrum_ref, green_ref, own_ref, swap_ref, c0_ref, c1_ref, c2_ref, keep_ref, give_ref, left_ref
):
    z, yh, core, x, yl = place_of_device()
    panel_rows, width = own_ref.shape[1:]
    blocks = [(ref, k) for ref in (c0_ref, c1_ref, c2_ref) for k in range(3)]
    fill_left(blocks, left_ref, x * 2 + yl, panel_rows)
    half = left_ref.shape[0] // 2
    begin = green_ref.shape[3] - half
    total = [spectrum_ref[0:1, :], spectrum_ref[1:2, :]]
    for k, screen_ref in enumerate((own_ref, swap_ref)):
        sums = (jnp.zeros((half, 128), jnp.float32),) * 2
        for tile in range(width // TILE):
            sums = add_tile(blocks, left_ref, screen_ref, tile, sums)
        total = added(total, sums, green_ref, k, begin, half)
    keep_ref[...] = jnp.where(core == 0, total[0], total[1])
    give_ref[...] = jnp.where(core == 0, total[1], total[0])


def last_kernel(prefactor, parts_ref, out_ref):
    z, yh = lax.axis_index("pb"), lax.axis_index("yh")
    total = jnp.sum(parts_ref[...], axis=0, keepdims=True)
    total = jnp.broadcast_to(total, (8, 128))
    real = pltpu.roll(total, (128 - (z * 2 + yh) * 4) % 128, 1)
    imag = pltpu.roll(real, 64, 1)
    out_ref[0] = -prefactor * imag[:1, :4]
    out_ref[1] = prefactor * real[:1, :4]


def in_memory(space, count):
    return [pl.BlockSpec(memory_space=space)] * count


def body(densities, screened, energies, occupied, kmq, offsets, weights):
    count_pb = lax.axis_size("pb")
    block = densities
    screen = screened[0, 0]
    rows = block.shape[2]
    count = 16 * rows

    first = [moved(block, count_pb, along_first(s)) for s in OFFSETS]
    second = [moved(block, count_pb, along_second(s)) for s in OFFSETS]
    swapped = moved(screen, count_pb, other_core)
    line = jnp.concatenate(first)
    rest = [moved(line, count_pb, along_second(s)) for s in OFFSETS]

    near_rows = 2 * NEAR * rows
    parameters = [
        pltpu.with_memory_space_constraint(value, pltpu.HBM)
        for value in (kmq, occupied, offsets, weights, energies, block, screen)
    ]
    own, green, spectrum = pl.pallas_call(
        near_kernel,
        out_shape=(
            pltpu.VMEM(screen.shape, screen.dtype),
            pltpu.VMEM((2, 2, 2, count, 128), jnp.float32),
            pltpu.VMEM((2, 128), jnp.float32),
        ),
        in_specs=in_memory(pltpu.HBM, 7) + in_memory(pltpu.VMEM, 7),
        out_specs=in_memory(pltpu.VMEM, 3),
        scratch_shapes=[
            pltpu.SMEM(kmq.shape, kmq.dtype),
            pltpu.SMEM(occupied.shape, occupied.dtype),
            pltpu.SMEM(offsets.shape, offsets.dtype),
            pltpu.SMEM(weights.shape, weights.dtype),
            pltpu.VMEM(energies.shape, energies.dtype),
            pltpu.VMEM(block.shape, block.dtype),
            pltpu.VMEM((near_rows, 2 * screen.shape[1]), jnp.bfloat16),
            pltpu.SemaphoreType.DMA((screen.shape[2] // TILE + 6,)),
        ],
        cost_estimate=pl.CostEstimate(
            flops=10**7, bytes_accessed=3 * 10**7, transcendentals=0
        ),
        compiler_params=pltpu.CompilerParams(vmem_limit_bytes=8 * 2**20),
        name="near",
    )(*parameters, *first, *second, swapped)

    keep, give = pl.pallas_call(
        far_kernel,
        out_shape=(jax.ShapeDtypeStruct((1, 128), jnp.float32),) * 2,
        in_specs=in_memory(pltpu.VMEM, 7),
        out_specs=in_memory(pltpu.VMEM, 2),
        scratch_shapes=[pltpu.VMEM((2 * 9 * rows, 2 * screen.shape[1]), jnp.bfloat16)],
        compiler_params=pltpu.CompilerParams(vmem_limit_bytes=8 * 2**20),
        name="far",
    )(spectrum, green, own, swapped, *rest)

    chip = keep + moved(give, count_pb, other_core)
    peers = count_pb * 16
    parts = lax.all_to_all(
        jnp.broadcast_to(chip, (peers, 1, 128)), SAME_CORE, 0, 0, tiled=True
    )
    return pl.pallas_call(
        functools.partial(last_kernel, 1.0 / (2.0 * math.pi * count_pb)),
        out_shape=jax.ShapeDtypeStruct((2, 1, 4), jnp.float32),
        in_specs=in_memory(pltpu.VMEM, 1),
        out_specs=pl.BlockSpec(memory_space=pltpu.VMEM),
        compiler_params=pltpu.CompilerParams(vmem_limit_bytes=2**20),
        name="last",
    )(parts.reshape(peers, 128))


def solution(mesh):
    torus = Mesh(mesh.devices.reshape(mesh.shape["pb"], 2, 2, 4, 2), AXES)
    return jax.shard_map(
        body,
        mesh=torus,
        in_specs=(
            P("pb", None, ("yh", "core", "x", "yl"), None),
            P("pb", ("yh", "core"), None, ("x", "yl"), None),
            P(),
            P(),
            P(),
            P(),
            P(),
        ),
        out_specs=P(None, None, ("pb", "yh", "core")),
        check_vma=False,
    )
```

```python
import functools
import math

import jax
import jax.numpy as jnp
from jax import lax
from jax.experimental import pallas as pl
from jax.experimental.pallas import tpu as pltpu
from jax.sharding import Mesh
from jax.sharding import PartitionSpec as P


AXES = ("pb", "yh", "core", "x", "yl")
SAME_CORE = ("pb", "yh", "x", "yl")
MASKS = (2, 1, 3)
FIRST_OF = (0, *MASKS) + (0, 0, 0) + MASKS * 3
SECOND_OF = (0, 0, 0, 0) + MASKS + (2,) * 3 + (1,) * 3 + (3,) * 3
NEAR = 7
BROADENING = 0.15
TILE = 512


def position(z, y, core, x):
    return (((z * 2 + y // 2) * 2 + core) * 4 + x) * 2 + y % 2


def moved(value, count_pb, place):
    pairs = []
    for z in range(count_pb):
        for y in range(4):
            for core in range(2):
                for x in range(4):
                    ny, ncore, nx = place(y, core, x)
                    pairs.append(
                        (position(z, y, core, x), position(z, ny, ncore, nx))
                    )
    return lax.ppermute(value, AXES, pairs)


def along_first(mask):
    return lambda y, core, x: (y, core, x ^ mask) if core == 0 else (y ^ mask, core, x)


def along_second(mask):
    return lambda y, core, x: (y ^ mask, core, x) if core == 0 else (y, core, x ^ mask)


def other_core(y, core, x):
    return (y, 1 - core, x)


def place_of_device():
    return [lax.axis_index(name) for name in AXES]


def stacked_rows(blocks, part, start, width):
    pieces = [ref[k, part, :, pl.ds(start, width)].astype(jnp.float32) for ref, k in blocks]
    return jnp.concatenate(pieces, axis=0)


def fill_left(blocks, left_ref, panel, panel_rows):
    start = pl.multiple_of(panel * panel_rows, panel_rows)
    real = stacked_rows(blocks, 0, start, panel_rows)
    imag = stacked_rows(blocks, 1, start, panel_rows)
    half = real.shape[0]
    left_ref[:half, :panel_rows] = real.astype(jnp.bfloat16)
    left_ref[:half, panel_rows:] = imag.astype(jnp.bfloat16)
    left_ref[half:, :panel_rows] = (-imag).astype(jnp.bfloat16)
    left_ref[half:, panel_rows:] = real.astype(jnp.bfloat16)


def add_tile(blocks, left_ref, screen_ref, tile, sums):
    start = pl.multiple_of(tile * TILE, TILE)
    half = left_ref.shape[0] // 2
    right = screen_ref[:, :, pl.ds(start, TILE)].reshape(left_ref.shape[1], TILE)
    product = jnp.dot(left_ref[...], right, preferred_element_type=jnp.float32)
    y_real, y_imag = product[:half], product[half:]
    real = stacked_rows(blocks, 0, start, TILE)
    imag = stacked_rows(blocks, 1, start, TILE)
    terms = (real * y_real - imag * y_imag, real * y_imag + imag * y_real)
    out = []
    for held, term in zip(sums, terms):
        for k in range(TILE // 128):
            held = held + term[:, k * 128 : (k + 1) * 128]
        out.append(held)
    return tuple(out)


def near_kernel(
    kmq_hbm,
    occupied_hbm,
    offsets_hbm,
    weights_hbm,
    energies_hbm,
    block_hbm,
    own_hbm,
    a0_ref,
    a1_ref,
    a2_ref,
    b0_ref,
    b1_ref,
    b2_ref,
    swap_ref,
    own_ref,
    green_ref,
    spectrum_ref,
    kmq_ref,
    occupied_ref,
    offsets_ref,
    weights_ref,
    energies_ref,
    block_ref,
    left_ref,
    sems,
):
    z, yh, core, x, yl = place_of_device()
    y = yh * 2 + yl
    panel_rows, width = own_hbm.shape[1:]
    tiles = width // TILE
    small = [
        pltpu.make_async_copy(src, dst, sems.at[tiles + k])
        for k, (src, dst) in enumerate(
            (
                (kmq_hbm, kmq_ref),
                (occupied_hbm, occupied_ref),
                (offsets_hbm, offsets_ref),
                (weights_hbm, weights_ref),
                (energies_hbm, energies_ref),
                (block_hbm, block_ref),
            )
        )
    ]
    large = []
    for tile in range(tiles):
        piece = pl.ds(tile * TILE, TILE)
        large.append(
            pltpu.make_async_copy(
                own_hbm.at[:, :, piece], own_ref.at[:, :, piece], sems.at[tile]
            )
        )
    for copy in small + large:
        copy.start()
    for copy in small:
        copy.wait()

    kpoint = kmq_ref[z]
    level_row = energies_ref[pl.ds(kpoint, 1), :]
    filled = occupied_ref[kpoint]
    rows = block_ref.shape[2]
    lanes = level_row.shape[1]
    columns, signs = [], []
    for first, second in zip(FIRST_OF, SECOND_OF):
        source_x = x ^ jnp.where(core == 0, first, second)
        source_y = y ^ jnp.where(core == 0, second, first)
        source = (source_y // 2 * 2 + core) * 8 + source_x * 2 + source_y % 2
        band = source * rows + lax.broadcasted_iota(jnp.int32, (rows, lanes), 0)
        match = lax.broadcasted_iota(jnp.int32, (rows, lanes), 1) == band
        picked = jnp.where(match, jnp.broadcast_to(level_row, (rows, lanes)), 0.0)
        columns.append(jnp.sum(picked, axis=1, keepdims=True))
        signs.append(jnp.where(band[:, :1] < filled, -1.0, 1.0))
    levels = jnp.concatenate(columns, axis=0)
    imag_part = BROADENING * jnp.concatenate(signs, axis=0)

    total_out = 128
    count = levels.shape[0]
    lane = lax.broadcasted_iota(jnp.int32, (count, total_out), 1)
    is_real = lane < 64
    within = lane % 64
    for k in range(2):
        freq = yh * 2 + jnp.where(k == 0, core, 1 - core)
        freq_shift = 4.0 * offsets_ref[freq].astype(jnp.float32) / total_out
        weight = weights_ref[freq]
        for target in range(2):
            index = (within // 4 * 2 + target) * 4 + within % 4
            omegas = -2.0 + 4.0 * index.astype(jnp.float32) / total_out
            real_part = omegas - freq_shift - levels
            denominator = real_part * real_part + imag_part * imag_part
            g_real = weight * (real_part / denominator)
            g_imag = weight * (-imag_part / denominator)
            green_ref[k, target, 0] = jnp.where(is_real, g_real, g_imag)
            green_ref[k, target, 1] = jnp.where(is_real, -g_imag, g_real)

    blocks = [
        (ref, 0)
        for ref in (block_ref, a0_ref, a1_ref, a2_ref, b0_ref, b1_ref, b2_ref)
    ]
    fill_left(blocks, left_ref, x * 2 + yl, panel_rows)
    half = left_ref.shape[0] // 2
    total = [jnp.zeros((1, total_out), jnp.float32) for _ in range(2)]
    for k, screen_ref in ((1, swap_ref), (0, own_ref)):
        sums = (jnp.zeros((half, 128), jnp.float32),) * 2
        for tile in range(tiles):
            if k == 0:
                large[tile].wait()
            sums = add_tile(blocks, left_ref, screen_ref, tile, sums)
        total = added(total, sums, green_ref, k, 0, half)
    spectrum_ref[0:1, :] = total[0]
    spectrum_ref[1:2, :] = total[1]


def added(total, sums, green_ref, k, begin, half):
    p_real = jnp.sum(sums[0], axis=1, keepdims=True)
    p_imag = jnp.sum(sums[1], axis=1, keepdims=True)
    out = []
    for target in range(2):
        u = green_ref[k, target, 0, begin : begin + half]
        v = green_ref[k, target, 1, begin : begin + half]
        out.append(total[target] + jnp.sum(p_real * u + p_imag * v, axis=0, keepdims=True))
    return out


def far_kernel(
    spectrum_ref, green_ref, own_ref, swap_ref, c0_ref, c1_ref, c2_ref, keep_ref, give_ref, left_ref
):
    _, _, core, x, yl = place_of_device()
    panel_rows, width = own_ref.shape[1:]
    blocks = [(ref, k) for ref in (c0_ref, c1_ref, c2_ref) for k in range(3)]
    fill_left(blocks, left_ref, x * 2 + yl, panel_rows)
    half = left_ref.shape[0] // 2
    begin = green_ref.shape[3] - half
    total = [spectrum_ref[0:1, :], spectrum_ref[1:2, :]]
    for k, screen_ref in enumerate((own_ref, swap_ref)):
        sums = (jnp.zeros((half, 128), jnp.float32),) * 2
        for tile in range(width // TILE):
            sums = add_tile(blocks, left_ref, screen_ref, tile, sums)
        total = added(total, sums, green_ref, k, begin, half)
    keep_ref[...] = jnp.where(core == 0, total[0], total[1])
    give_ref[...] = jnp.where(core == 0, total[1], total[0])


def last_kernel(prefactor, parts_ref, out_ref):
    z, yh = lax.axis_index("pb"), lax.axis_index("yh")
    total = jnp.sum(parts_ref[...], axis=0, keepdims=True)
    total = jnp.broadcast_to(total, (8, 128))
    real = pltpu.roll(total, (128 - (z * 2 + yh) * 4) % 128, 1)
    imag = pltpu.roll(real, 64, 1)
    out_ref[0] = -prefactor * imag[:1, :4]
    out_ref[1] = prefactor * real[:1, :4]


def in_memory(space, count):
    return [pl.BlockSpec(memory_space=space)] * count


def body(densities, screened, energies, occupied, kmq, offsets, weights):
    count_pb = lax.axis_size("pb")
    block = densities
    screen = screened[0, 0]
    rows = block.shape[2]
    count = 16 * rows

    swapped = moved(screen, count_pb, other_core)
    first = [moved(block, count_pb, along_first(m)) for m in MASKS]
    second = [moved(block, count_pb, along_second(m)) for m in MASKS]
    line = jnp.concatenate(first)
    rest = [moved(line, count_pb, along_second(m)) for m in MASKS]

    near_rows = 2 * NEAR * rows
    parameters = [
        pltpu.with_memory_space_constraint(value, pltpu.HBM)
        for value in (kmq, occupied, offsets, weights, energies, block, screen)
    ]
    near = pl.pallas_call(
        near_kernel,
        out_shape=(
            pltpu.VMEM(screen.shape, screen.dtype),
            pltpu.VMEM((2, 2, 2, count, 128), jnp.float32),
            pltpu.VMEM((2, 128), jnp.float32),
        ),
        in_specs=in_memory(pltpu.HBM, 7) + in_memory(pltpu.VMEM, 7),
        out_specs=in_memory(pltpu.VMEM, 3),
        scratch_shapes=[
            pltpu.SMEM(kmq.shape, kmq.dtype),
            pltpu.SMEM(occupied.shape, occupied.dtype),
            pltpu.SMEM(offsets.shape, offsets.dtype),
            pltpu.SMEM(weights.shape, weights.dtype),
            pltpu.VMEM(energies.shape, energies.dtype),
            pltpu.VMEM(block.shape, block.dtype),
            pltpu.VMEM((near_rows, 2 * screen.shape[1]), jnp.bfloat16),
            pltpu.SemaphoreType.DMA((screen.shape[2] // TILE + 6,)),
        ],
        cost_estimate=pl.CostEstimate(
            flops=10**7, bytes_accessed=3 * 10**7, transcendentals=0
        ),
        compiler_params=pltpu.CompilerParams(vmem_limit_bytes=8 * 2**20),
        name="near",
    )
    own, green, spectrum = near(*parameters, *first, *second, swapped)

    keep, give = pl.pallas_call(
        far_kernel,
        out_shape=(jax.ShapeDtypeStruct((1, 128), jnp.float32),) * 2,
        in_specs=in_memory(pltpu.VMEM, 7),
        out_specs=in_memory(pltpu.VMEM, 2),
        scratch_shapes=[pltpu.VMEM((2 * 9 * rows, 2 * screen.shape[1]), jnp.bfloat16)],
        compiler_params=pltpu.CompilerParams(vmem_limit_bytes=8 * 2**20),
        name="far",
    )(spectrum, green, own, swapped, *rest)

    chip = keep + moved(give, count_pb, other_core)
    peers = count_pb * 16
    parts = lax.all_to_all(
        jnp.broadcast_to(chip, (peers, 1, 128)), SAME_CORE, 0, 0, tiled=True
    )
    return pl.pallas_call(
        functools.partial(last_kernel, 1.0 / (2.0 * math.pi * count_pb)),
        out_shape=jax.ShapeDtypeStruct((2, 1, 4), jnp.float32),
        in_specs=in_memory(pltpu.VMEM, 1),
        out_specs=pl.BlockSpec(memory_space=pltpu.VMEM),
        compiler_params=pltpu.CompilerParams(vmem_limit_bytes=2**20),
        name="last",
    )(parts.reshape(peers, 128))


def solution(mesh):
    torus = Mesh(mesh.devices.reshape(mesh.shape["pb"], 2, 2, 4, 2), AXES)
    return jax.shard_map(
        body,
        mesh=torus,
        in_specs=(
            P("pb", None, ("yh", "core", "x", "yl"), None),
            P("pb", ("yh", "core"), None, ("x", "yl"), None),
            P(),
            P(),
            P(),
            P(),
            P(),
        ),
        out_specs=P(None, None, ("pb", "yh", "core")),
        check_vma=False,
    )
```

```python
import functools
import math

import jax
import jax.numpy as jnp
from jax import lax
from jax.experimental import pallas as pl
from jax.experimental.pallas import tpu as pltpu
from jax.sharding import Mesh
from jax.sharding import PartitionSpec as P


AXES = ("pb", "yh", "core", "x", "yl")
SAME_CORE = ("pb", "yh", "x", "yl")
MASKS = (2, 1, 3)
FIRST_OF = MASKS + (0, 0, 0) + (0,) + (2, 3, 2, 1, 2, 1, 1, 3, 3)
SECOND_OF = (0, 0, 0) + MASKS + (0,) + (1, 1, 3, 3, 2, 2, 1, 2, 3)
NEAR = 6
BROADENING = 0.15
TILE = 512


def position(z, y, core, x):
    return (((z * 2 + y // 2) * 2 + core) * 4 + x) * 2 + y % 2


def moved(value, count_pb, place):
    pairs = []
    for z in range(count_pb):
        for y in range(4):
            for core in range(2):
                for x in range(4):
                    ny, ncore, nx = place(y, core, x)
                    pairs.append(
                        (position(z, y, core, x), position(z, ny, ncore, nx))
                    )
    return lax.ppermute(value, AXES, pairs)


def along_first(mask):
    return lambda y, core, x: (y, core, x ^ mask) if core == 0 else (y ^ mask, core, x)


def along_second(mask):
    return lambda y, core, x: (y ^ mask, core, x) if core == 0 else (y, core, x ^ mask)


def other_core(y, core, x):
    return (y, 1 - core, x)


def place_of_device():
    return [lax.axis_index(name) for name in AXES]


def stacked_rows(blocks, part, start, width):
    pieces = [ref[k, part, :, pl.ds(start, width)].astype(jnp.float32) for ref, k in blocks]
    return jnp.concatenate(pieces, axis=0)


def fill_left(blocks, left_ref, panel, panel_rows):
    start = pl.multiple_of(panel * panel_rows, panel_rows)
    real = stacked_rows(blocks, 0, start, panel_rows)
    imag = stacked_rows(blocks, 1, start, panel_rows)
    half = real.shape[0]
    left_ref[:half, :panel_rows] = real.astype(jnp.bfloat16)
    left_ref[:half, panel_rows:] = imag.astype(jnp.bfloat16)
    left_ref[half:, :panel_rows] = (-imag).astype(jnp.bfloat16)
    left_ref[half:, panel_rows:] = real.astype(jnp.bfloat16)


def add_tile(blocks, left_ref, screen_ref, tile, sums):
    start = pl.multiple_of(tile * TILE, TILE)
    half = left_ref.shape[0] // 2
    right = screen_ref[:, :, pl.ds(start, TILE)].reshape(left_ref.shape[1], TILE)
    product = jnp.dot(left_ref[...], right, preferred_element_type=jnp.float32)
    y_real, y_imag = product[:half], product[half:]
    real = stacked_rows(blocks, 0, start, TILE)
    imag = stacked_rows(blocks, 1, start, TILE)
    terms = (real * y_real - imag * y_imag, real * y_imag + imag * y_real)
    out = []
    for held, term in zip(sums, terms):
        for k in range(TILE // 128):
            held = held + term[:, k * 128 : (k + 1) * 128]
        out.append(held)
    return tuple(out)


def near_kernel(
    kmq_hbm,
    occupied_hbm,
    offsets_hbm,
    weights_hbm,
    energies_hbm,
    block_hbm,
    own_hbm,
    a0_ref,
    a1_ref,
    a2_ref,
    b0_ref,
    b1_ref,
    b2_ref,
    swap_ref,
    own_ref,
    block_ref,
    green_ref,
    spectrum_ref,
    kmq_ref,
    occupied_ref,
    offsets_ref,
    weights_ref,
    energies_ref,
    left_ref,
    sems,
):
    z, yh, core, x, yl = place_of_device()
    y = yh * 2 + yl
    panel_rows, width = own_hbm.shape[1:]
    tiles = width // TILE
    large = []
    for tile in range(tiles):
        piece = pl.ds(tile * TILE, TILE)
        large.append(
            pltpu.make_async_copy(
                own_hbm.at[:, :, piece], own_ref.at[:, :, piece], sems.at[tile]
            )
        )
    small = [
        pltpu.make_async_copy(src, dst, sems.at[tiles + k])
        for k, (src, dst) in enumerate(
            (
                (kmq_hbm, kmq_ref),
                (occupied_hbm, occupied_ref),
                (offsets_hbm, offsets_ref),
                (weights_hbm, weights_ref),
                (energies_hbm, energies_ref),
                (block_hbm, block_ref),
            )
        )
    ]
    for copy in large + small:
        copy.start()
    blocks = [(ref, 0) for ref in (a0_ref, a1_ref, a2_ref, b0_ref, b1_ref, b2_ref)]
    fill_left(blocks, left_ref, x * 2 + yl, panel_rows)
    half = left_ref.shape[0] // 2
    sums = []
    for late, screen_ref in ((False, swap_ref), (True, own_ref)):
        held = (jnp.zeros((half, 128), jnp.float32),) * 2
        for tile in range(tiles):
            if late:
                large[tile].wait()
            held = add_tile(blocks, left_ref, screen_ref, tile, held)
        sums.append(held)

    for copy in small:
        copy.wait()
    kpoint = kmq_ref[z]
    level_row = energies_ref[pl.ds(kpoint, 1), :]
    filled = occupied_ref[kpoint]
    rows = block_ref.shape[2]
    lanes = level_row.shape[1]
    columns, signs = [], []
    for first, second in zip(FIRST_OF, SECOND_OF):
        source_x = x ^ jnp.where(core == 0, first, second)
        source_y = y ^ jnp.where(core == 0, second, first)
        source = (source_y // 2 * 2 + core) * 8 + source_x * 2 + source_y % 2
        band = source * rows + lax.broadcasted_iota(jnp.int32, (rows, lanes), 0)
        match = lax.broadcasted_iota(jnp.int32, (rows, lanes), 1) == band
        picked = jnp.where(match, jnp.broadcast_to(level_row, (rows, lanes)), 0.0)
        columns.append(jnp.sum(picked, axis=1, keepdims=True))
        signs.append(jnp.where(band[:, :1] < filled, -1.0, 1.0))
    levels = jnp.concatenate(columns, axis=0)
    imag_part = BROADENING * jnp.concatenate(signs, axis=0)

    total_out = 128
    count = levels.shape[0]
    lane = lax.broadcasted_iota(jnp.int32, (count, total_out), 1)
    is_real = lane < 64
    within = lane % 64
    for k in range(2):
        freq = yh * 2 + jnp.where(k == 0, core, 1 - core)
        freq_shift = 4.0 * offsets_ref[freq].astype(jnp.float32) / total_out
        weight = weights_ref[freq]
        for target in range(2):
            index = (within // 4 * 2 + target) * 4 + within % 4
            omegas = -2.0 + 4.0 * index.astype(jnp.float32) / total_out
            real_part = omegas - freq_shift - levels
            denominator = real_part * real_part + imag_part * imag_part
            g_real = weight * (real_part / denominator)
            g_imag = weight * (-imag_part / denominator)
            green_ref[k, target, 0] = jnp.where(is_real, g_real, g_imag)
            green_ref[k, target, 1] = jnp.where(is_real, -g_imag, g_real)

    total = [jnp.zeros((1, total_out), jnp.float32) for _ in range(2)]
    for k, held in ((1, sums[0]), (0, sums[1])):
        total = added(total, held, green_ref, k, 0, half)
    spectrum_ref[0:1, :] = total[0]
    spectrum_ref[1:2, :] = total[1]


def added(total, sums, green_ref, k, begin, half):
    p_real = jnp.sum(sums[0], axis=1, keepdims=True)
    p_imag = jnp.sum(sums[1], axis=1, keepdims=True)
    out = []
    for target in range(2):
        u = green_ref[k, target, 0, begin : begin + half]
        v = green_ref[k, target, 1, begin : begin + half]
        out.append(total[target] + jnp.sum(p_real * u + p_imag * v, axis=0, keepdims=True))
    return out


def far_kernel(
    spectrum_ref, green_ref, own_ref, swap_ref, *refs
):
    *parts, keep_ref, give_ref, left_ref = refs
    _, _, core, x, yl = place_of_device()
    panel_rows, width = own_ref.shape[1:]
    blocks = [(ref, k) for ref in parts for k in range(ref.shape[0])]
    fill_left(blocks, left_ref, x * 2 + yl, panel_rows)
    half = left_ref.shape[0] // 2
    begin = green_ref.shape[3] - half
    total = [spectrum_ref[0:1, :], spectrum_ref[1:2, :]]
    for k, screen_ref in enumerate((own_ref, swap_ref)):
        sums = (jnp.zeros((half, 128), jnp.float32),) * 2
        for tile in range(width // TILE):
            sums = add_tile(blocks, left_ref, screen_ref, tile, sums)
        total = added(total, sums, green_ref, k, begin, half)
    keep_ref[...] = jnp.where(core == 0, total[0], total[1])
    give_ref[...] = jnp.where(core == 0, total[1], total[0])


def last_kernel(prefactor, parts_ref, out_ref):
    z, yh = lax.axis_index("pb"), lax.axis_index("yh")
    total = jnp.sum(parts_ref[...], axis=0, keepdims=True)
    total = jnp.broadcast_to(total, (8, 128))
    real = pltpu.roll(total, (128 - (z * 2 + yh) * 4) % 128, 1)
    imag = pltpu.roll(real, 64, 1)
    out_ref[0] = -prefactor * imag[:1, :4]
    out_ref[1] = prefactor * real[:1, :4]


def in_memory(space, count):
    return [pl.BlockSpec(memory_space=space)] * count


def body(densities, screened, energies, occupied, kmq, offsets, weights):
    count_pb = lax.axis_size("pb")
    block = densities
    screen = screened[0, 0]
    rows = block.shape[2]
    count = 16 * rows

    swapped = moved(screen, count_pb, other_core)
    first = [moved(block, count_pb, along_first(m)) for m in MASKS]
    second = [moved(block, count_pb, along_second(m)) for m in MASKS]
    a, b = dict(zip(MASKS, first)), dict(zip(MASKS, second))
    pair = lambda one, two: jnp.concatenate([one, two])
    rest = [
        moved(pair(a[2], a[3]), count_pb, along_second(1)),
        moved(pair(a[2], a[1]), count_pb, along_second(3)),
        moved(a[2], count_pb, along_second(2)),
        moved(pair(b[2], b[1]), count_pb, along_first(1)),
        moved(pair(b[2], b[3]), count_pb, along_first(3)),
    ]

    near_rows = 2 * NEAR * rows
    parameters = [
        pltpu.with_memory_space_constraint(value, pltpu.HBM)
        for value in (kmq, occupied, offsets, weights, energies, block, screen)
    ]
    near = pl.pallas_call(
        near_kernel,
        out_shape=(
            pltpu.VMEM(screen.shape, screen.dtype),
            pltpu.VMEM(block.shape, block.dtype),
            pltpu.VMEM((2, 2, 2, count, 128), jnp.float32),
            pltpu.VMEM((2, 128), jnp.float32),
        ),
        in_specs=in_memory(pltpu.HBM, 7) + in_memory(pltpu.VMEM, 7),
        out_specs=in_memory(pltpu.VMEM, 4),
        scratch_shapes=[
            pltpu.SMEM(kmq.shape, kmq.dtype),
            pltpu.SMEM(occupied.shape, occupied.dtype),
            pltpu.SMEM(offsets.shape, offsets.dtype),
            pltpu.SMEM(weights.shape, weights.dtype),
            pltpu.VMEM(energies.shape, energies.dtype),
            pltpu.VMEM((near_rows, 2 * screen.shape[1]), jnp.bfloat16),
            pltpu.SemaphoreType.DMA((screen.shape[2] // TILE + 6,)),
        ],
        cost_estimate=pl.CostEstimate(
            flops=10**7, bytes_accessed=3 * 10**7, transcendentals=0
        ),
        compiler_params=pltpu.CompilerParams(vmem_limit_bytes=8 * 2**20),
        name="near",
    )
    own, held, green, spectrum = near(*parameters, *first, *second, swapped)

    keep, give = pl.pallas_call(
        far_kernel,
        out_shape=(jax.ShapeDtypeStruct((1, 128), jnp.float32),) * 2,
        in_specs=in_memory(pltpu.VMEM, 5 + len(rest)),
        out_specs=in_memory(pltpu.VMEM, 2),
        scratch_shapes=[pltpu.VMEM((2 * 10 * rows, 2 * screen.shape[1]), jnp.bfloat16)],
        compiler_params=pltpu.CompilerParams(vmem_limit_bytes=8 * 2**20),
        name="far",
    )(spectrum, green, own, swapped, held, *rest)

    chip = keep + moved(give, count_pb, other_core)
    peers = count_pb * 16
    parts = lax.all_to_all(
        jnp.broadcast_to(chip, (peers, 1, 128)), SAME_CORE, 0, 0, tiled=True
    )
    return pl.pallas_call(
        functools.partial(last_kernel, 1.0 / (2.0 * math.pi * count_pb)),
        out_shape=jax.ShapeDtypeStruct((2, 1, 4), jnp.float32),
        in_specs=in_memory(pltpu.VMEM, 1),
        out_specs=pl.BlockSpec(memory_space=pltpu.VMEM),
        compiler_params=pltpu.CompilerParams(vmem_limit_bytes=2**20),
        name="last",
    )(parts.reshape(peers, 128))


def solution(mesh):
    torus = Mesh(mesh.devices.reshape(mesh.shape["pb"], 2, 2, 4, 2), AXES)
    return jax.shard_map(
        body,
        mesh=torus,
        in_specs=(
            P("pb", None, ("yh", "core", "x", "yl"), None),
            P("pb", ("yh", "core"), None, ("x", "yl"), None),
            P(),
            P(),
            P(),
            P(),
            P(),
        ),
        out_specs=P(None, None, ("pb", "yh", "core")),
        check_vma=False,
    )
```
